256 devices in a mesh: slab: 128 (over z, y_lo, x, core), chan: 2 (over y_hi).
Axes of the slice: x: 4, y: 4 (y_hi: 2, y_lo: 2; y = y_hi * 2 + y_lo), z: 8, core: 2. Of those that a mesh axis runs over, the one named last changes fastest.
Arguments:
- species: int32 [32768], P('slab'), may hold values from 0 to 4
- atom_count: int32 [128], P('slab'), may hold values from 192 to 256, as said below
- halo_index: int32 [128, 2, 128], P('slab'), may hold values from 0 to 255, as said below
- edge_count: int32 [128, 2], P('slab'), may hold values from 512 to 12288, as said below
- inner_edges: int32 [2, 1572864], P(None, 'slab'), may hold values from 0 to 255, as said below
- outer_edges: int32 [2, 524288], P(None, 'slab'), may hold values from 0 to 255, as said below
- inner_vec: float32 [3, 1572864], P(None, 'slab'), may hold values from -4.8 to 4.8, as said below
- outer_vec: float32 [3, 524288], P(None, 'slab'), may hold values from -4.8 to 4.8, as said below
- embed_table: bfloat16 [64, 5], replicated, may hold values from -6 to 6
- radial_in: bfloat16 [2, 64, 8], replicated, may hold values from -2 to 2
- radial_mid: bfloat16 [2, 64, 64], replicated, may hold values from -0.75 to 0.75
- radial_out: bfloat16 [2, 10, 64, 64], P(None, None, 'chan'), may hold values from -0.75 to 0.75
- mix_in: bfloat16 [2, 3, 64, 64], P(None, None, 'chan'), may hold values from -0.75 to 0.75
- mix_scalar: bfloat16 [2, 192, 64], replicated, may hold values from -0.75 to 0.75
- mix_irrep: bfloat16 [2, 2, 64, 64], replicated, may hold values from -0.75 to 0.75
- readout: float32 [64], replicated, may hold values from -0.75 to 0.75
- species_energy: float32 [5], replicated, may hold values from -6 to -2
Outputs:
- node_state: float32 [9, 64, 32768], P(None, None, 'slab')
- atom_energy: float32 [32768], P('slab')
- mean_energy: float32 [], replicated
The draws below stay inside these ranges and needn't reach their ends.
Inputs may be any that keep to these rules, and one draw needn't show every extreme that they name: `atom_count`: each slab holds between 192 and 256 live atoms (rounded down), live slots first; some slab holds exactly 256. `halo_index`: every entry names a live atom of its own slab. `edge_count`: column 0 lies between 1536 and 12288, column 1 between 512 and 4096 (rounded down); live slots come first in each list; each column reaches its most in some slab. `inner_edges`: both rows name live atoms of the same slab, in every slot. `outer_edges`: row 0 lies below 256; row 1 names a live atom of the slab, in every slot. `inner_vec`: every displacement is shorter than 4.8; nearly all are 0.9 or longer, and a rare few are shorter. `outer_vec`: every displacement is shorter than 4.8; nearly all are 0.9 or longer, and a rare few are shorter.
All inputs are finite; a program needn't handle non-finite values.
Results may differ from the reference program's by a relative error of at most 0.00045.
Values may be sent and summed in bfloat16 or wider, within the bound.
A program may use at most 64 MiB of HBM per device.

```python
import math
import jax
import jax.numpy as jnp
import numpy as np
from jax import lax

C = 64
NB = 8
RH = 64
NPATH = 10
NSPEC = 5
LAYERS = 2
A_DEV = 256
H_DEV = 128
E_IN = 12288
E_OUT = 4096
ATOMS = 32768


def slab_atoms(key):
    base_key = jax.random.fold_in(key, 11)
    slab_total = ATOMS // A_DEV
    counts = jax.random.randint(base_key, (slab_total,), 3 * A_DEV // 4, A_DEV + 1)
    fullest = jax.random.randint(jax.random.fold_in(base_key, 1), (), 0, slab_total)
    return jnp.where(jnp.arange(slab_total) == fullest, A_DEV, counts).astype(jnp.int32)


def live_edges(key, salt, slots):
    base_key = jax.random.fold_in(key, salt)
    slab_total = ATOMS // A_DEV
    counts = jax.random.randint(base_key, (slab_total,), slots // 8, slots + 1)
    fullest = jax.random.randint(jax.random.fold_in(base_key, 1), (), 0, slab_total)
    return jnp.where(jnp.arange(slab_total) == fullest, slots, counts).astype(jnp.int32)


def displacement(key, salt, slots):
    base_key = jax.random.fold_in(key, salt)
    total = slots * (ATOMS // A_DEV)
    heading = jax.random.normal(jax.random.fold_in(base_key, 1), (3, total), jnp.float32)
    radius = jax.random.uniform(jax.random.fold_in(base_key, 2), (total,), jnp.float32, 0.9, 4.8)
    scale = radius / jnp.sqrt(jnp.sum(heading * heading, axis=0) + 0.001)
    return heading * scale[None, :]


def draw_atom_count(key, part):
    return slab_atoms(key)


def draw_halo_index(key, part):
    counts = slab_atoms(key)
    slab_total = ATOMS // A_DEV
    return jax.random.randint(jax.random.fold_in(key, 21), (slab_total, 2, H_DEV), 0, counts[:, None, None]).astype(jnp.int32)


def draw_edge_count(key, part):
    return jnp.stack([live_edges(key, 31, E_IN), live_edges(key, 41, E_OUT)], axis=1)


def draw_inner_edges(key, part):
    counts = slab_atoms(key)
    slab_total = ATOMS // A_DEV
    repeated = jnp.repeat(counts, E_IN, total_repeat_length=slab_total * E_IN)
    return jax.random.randint(jax.random.fold_in(key, 51), (2, slab_total * E_IN), 0, repeated[None, :]).astype(jnp.int32)


def draw_outer_edges(key, part):
    counts = slab_atoms(key)
    slab_total = ATOMS // A_DEV
    repeated = jnp.repeat(counts, E_OUT, total_repeat_length=slab_total * E_OUT)
    halo_slot = jax.random.randint(jax.random.fold_in(key, 61), (slab_total * E_OUT,), 0, 2 * H_DEV)
    targets = jax.random.randint(jax.random.fold_in(key, 62), (slab_total * E_OUT,), 0, repeated)
    return jnp.stack([halo_slot, targets], axis=0).astype(jnp.int32)


def draw_inner_vec(key, part):
    return displacement(key, 71, E_IN)


def draw_outer_vec(key, part):
    return displacement(key, 81, E_OUT)


def with_ends(entries, key, least, largest):
    longest = entries.shape.index(max(entries.shape))
    spots = []
    for shift in (0, 1):
        where = [jax.random.randint(jax.random.fold_in(key, axis), (), 0, length) for axis, length in enumerate(entries.shape)]
        where[longest] = (where[longest] + shift) % entries.shape[longest]
        spots.append(tuple(where))
    return entries.at[spots[0]].set(least).at[spots[1]].set(largest)


def block_scale(key, extent, cuts, low, largest):
    def one(dim, shards_of):
        draws = jax.random.uniform(jax.random.fold_in(jax.random.fold_in(key, 6), dim), (shards_of,), jnp.float32, low / len(cuts), largest / len(cuts))
        return jnp.repeat(jnp.exp(draws), extent[dim] // shards_of).reshape((-1,) + (1,) * (len(extent) - dim - 1))

    level = one(*cuts[0])
    for cut in cuts[1:]:
        level = level * one(*cut)
    return level


def rank_bounds(amount, lean):
    weights = [(1 << 20) // math.isqrt(grade ** lean) + 1 for grade in range(1, amount + 1)]
    width = 1 + sum(weights) // (1 << 30)
    return np.cumsum(np.array([max(1, weight // width) for weight in weights]))


def ranked_ids(own_key, extent, count, skew):
    listing = rank_bounds(count, skew)
    pick = jax.random.randint(jax.random.fold_in(own_key, 1), extent, 0, int(listing[count - 1]))
    grade = jnp.searchsorted(jnp.asarray(listing, jnp.int32), pick, side="right")
    return jax.random.permutation(jax.random.fold_in(own_key, 2), count)[grade].astype(jnp.int32)


def centred(rng, extent, width, reach, cuts=(), kind=jnp.bfloat16):
    gain = block_scale(rng, extent, cuts, -0.22, 0.18) if cuts else 1.0
    values = jax.random.normal(rng, extent, jnp.float32) * width * gain
    return jnp.minimum(jnp.maximum(values, -reach), reach).astype(kind)


def setup_inputs(seed: int = 0) -> dict:
    seeds = jax.random.split(jax.random.key(seed), 18)
    return {
        "species": with_ends(ranked_ids(seeds[0], (ATOMS,), NSPEC, 2), jax.random.fold_in(seeds[0], 3), 0, NSPEC - 1).astype(jnp.int32),
        "atom_count": draw_atom_count(jax.random.fold_in(seeds[17], 71), 0),
        "halo_index": draw_halo_index(jax.random.fold_in(seeds[17], 71), 0),
        "edge_count": draw_edge_count(jax.random.fold_in(seeds[17], 71), 0),
        "inner_edges": draw_inner_edges(jax.random.fold_in(seeds[17], 71), 0),
        "outer_edges": draw_outer_edges(jax.random.fold_in(seeds[17], 71), 0),
        "inner_vec": draw_inner_vec(jax.random.fold_in(seeds[17], 71), 0),
        "outer_vec": draw_outer_vec(jax.random.fold_in(seeds[17], 71), 0),
        "embed_table": centred(seeds[8], (C, NSPEC), 1.0, 6.0),
        "radial_in": centred(seeds[9], (LAYERS, RH, NB), NB ** -0.5, 2.0),
        "radial_mid": centred(seeds[10], (LAYERS, RH, RH), RH ** -0.5, 0.75),
        "radial_out": centred(seeds[11], (LAYERS, NPATH, C, RH), RH ** -0.5, 0.75, ((2, 2),)),
        "mix_in": centred(seeds[12], (LAYERS, 3, C, C), C ** -0.5, 0.75, ((2, 2),)),
        "mix_scalar": centred(seeds[13], (LAYERS, 3 * C, C), C ** -0.5, 0.75),
        "mix_irrep": centred(seeds[14], (LAYERS, 2, C, C), C ** -0.5, 0.75),
        "readout": centred(seeds[15], (C,), C ** -0.5, 0.75, (), jnp.float32),
        "species_energy": jnp.clip(jax.random.uniform(seeds[16], (NSPEC,), jnp.float32, -6.0, -2.0), -6.0, -2.0),
    }


cutoff = 5.0
neighbour_norm = 1.0 / math.sqrt(48.0)
root_three = math.sqrt(3.0)
half_root = 0.5 * math.sqrt(3.0)

def geometry(vectors, basis_total):
    squared = lax.optimization_barrier(jnp.sum(vectors * vectors, axis=0))
    length = jnp.sqrt(squared)
    softened = jnp.sqrt(squared + 0.25)
    directions = vectors / softened[None, :]
    fraction = jnp.minimum(length / cutoff, 1.0)
    envelope = 1.0 - 28.0 * fraction ** 6 + 48.0 * fraction ** 7 - 21.0 * fraction ** 8
    orders = jnp.arange(1, basis_total + 1, dtype=jnp.float32)[:, None]
    bessel = math.sqrt(2.0 / cutoff) * jnp.sin(orders * (math.pi / cutoff) * length[None, :]) / softened[None, :] * envelope[None, :]
    return (directions, bessel)

def edge_messages(source, directions, bessel, live_mask, layer_weights):
    first_layer, middle_layer, last_layer = layer_weights
    hidden = jax.nn.silu(jnp.dot(first_layer, bessel.astype(jnp.bfloat16), preferred_element_type=jnp.float32)).astype(jnp.bfloat16)
    hidden = jax.nn.silu(jnp.dot(middle_layer, hidden, preferred_element_type=jnp.float32)).astype(jnp.bfloat16)
    path_total, channels, breadth = last_layer.shape
    weights = jnp.dot(last_layer.reshape(path_total * channels, breadth), hidden, preferred_element_type=jnp.float32)
    weights = weights.reshape(path_total, channels, hidden.shape[1])
    features = source.astype(jnp.float32)
    scalar_in = features[0]
    vector_in = [features[1], features[2], features[3]]
    tensor_in = [features[4], features[5], features[6], features[7], features[8]]
    unit_parts = [directions[0][None, :], directions[1][None, :], directions[2][None, :]]
    unit_square = unit_parts[0] * unit_parts[0] + unit_parts[1] * unit_parts[1] + unit_parts[2] * unit_parts[2]
    harmonic = [root_three * unit_parts[0] * unit_parts[1], root_three * unit_parts[1] * unit_parts[2], 0.5 * (3.0 * unit_parts[2] * unit_parts[2] - unit_square), root_three * unit_parts[0] * unit_parts[2], half_root * (unit_parts[0] * unit_parts[0] - unit_parts[1] * unit_parts[1])]
    vector_along = vector_in[0] * unit_parts[0] + vector_in[1] * unit_parts[1] + vector_in[2] * unit_parts[2]
    tensor_along = tensor_in[0] * harmonic[0] + tensor_in[1] * harmonic[1] + tensor_in[2] * harmonic[2] + tensor_in[3] * harmonic[3] + tensor_in[4] * harmonic[4]
    out_scalar = weights[0] * scalar_in + weights[1] * tensor_along + weights[2] * vector_along
    cross_term = [vector_in[1] * unit_parts[2] - vector_in[2] * unit_parts[1], vector_in[2] * unit_parts[0] - vector_in[0] * unit_parts[2], vector_in[0] * unit_parts[1] - vector_in[1] * unit_parts[0]]
    gradient = [0.5 * (root_three * tensor_in[0] * unit_parts[1] - tensor_in[2] * unit_parts[0] + root_three * tensor_in[3] * unit_parts[2] + root_three * tensor_in[4] * unit_parts[0]), 0.5 * (root_three * tensor_in[0] * unit_parts[0] + root_three * tensor_in[1] * unit_parts[2] - tensor_in[2] * unit_parts[1] - root_three * tensor_in[4] * unit_parts[1]), 0.5 * (root_three * tensor_in[1] * unit_parts[1] + 2.0 * tensor_in[2] * unit_parts[2] + root_three * tensor_in[3] * unit_parts[0])]
    out_vector = [weights[3] * scalar_in * unit_parts[0] + weights[4] * vector_in[0] + weights[5] * cross_term[0] + weights[6] * gradient[0], weights[3] * scalar_in * unit_parts[1] + weights[4] * vector_in[1] + weights[5] * cross_term[1] + weights[6] * gradient[1], weights[3] * scalar_in * unit_parts[2] + weights[4] * vector_in[2] + weights[5] * cross_term[2] + weights[6] * gradient[2]]
    symmetric = [half_root * (vector_in[0] * unit_parts[1] + vector_in[1] * unit_parts[0]), half_root * (vector_in[1] * unit_parts[2] + vector_in[2] * unit_parts[1]), 0.5 * (3.0 * vector_in[2] * unit_parts[2] - vector_along), half_root * (vector_in[0] * unit_parts[2] + vector_in[2] * unit_parts[0]), half_root * (vector_in[0] * unit_parts[0] - vector_in[1] * unit_parts[1])]
    out_tensor = [weights[7] * scalar_in * harmonic[0] + weights[8] * tensor_in[0] + weights[9] * symmetric[0], weights[7] * scalar_in * harmonic[1] + weights[8] * tensor_in[1] + weights[9] * symmetric[1], weights[7] * scalar_in * harmonic[2] + weights[8] * tensor_in[2] + weights[9] * symmetric[2], weights[7] * scalar_in * harmonic[3] + weights[8] * tensor_in[3] + weights[9] * symmetric[3], weights[7] * scalar_in * harmonic[4] + weights[8] * tensor_in[4] + weights[9] * symmetric[4]]
    stacked = jnp.stack([out_scalar] + out_vector + out_tensor)
    return stacked * live_mask[None, None, :]

def mix_channels(weights, rounded):
    scalar_part = jnp.dot(weights[0], rounded[0], preferred_element_type=jnp.float32)[None]
    vector_part = jnp.einsum('oi,kia->koa', weights[1].astype(jnp.float32), rounded[1:4].astype(jnp.float32))
    tensor_part = jnp.einsum('oi,kia->koa', weights[2].astype(jnp.float32), rounded[4:9].astype(jnp.float32))
    return jnp.concatenate([scalar_part, vector_part, tensor_part], axis=0)

def gate_update(aggregated, scalar_weight, irrep_weight):
    channels = aggregated.shape[1]
    mixed_scalar = jnp.dot(scalar_weight, aggregated[0], preferred_element_type=jnp.float32)
    mixed_vector = jnp.einsum('oi,kia->koa', irrep_weight[0].astype(jnp.float32), aggregated[1:4].astype(jnp.float32))
    mixed_tensor = jnp.einsum('oi,kia->koa', irrep_weight[1].astype(jnp.float32), aggregated[4:9].astype(jnp.float32))
    new_scalar = jax.nn.silu(mixed_scalar[:channels])[None]
    new_vector = jax.nn.sigmoid(mixed_scalar[channels:2 * channels])[None] * mixed_vector
    new_tensor = jax.nn.sigmoid(mixed_scalar[2 * channels:])[None] * mixed_tensor
    return jnp.concatenate([new_scalar, new_vector, new_tensor], axis=0)

def reference(species, atom_count, halo_index, edge_count, inner_edges, outer_edges, inner_vec, outer_vec, embed_table, radial_in, radial_mid, radial_out, mix_in, mix_scalar, mix_irrep, readout, species_energy):
    slab_total = ATOMS // A_DEV
    onehot = species[None, :] == jnp.arange(NSPEC, dtype=jnp.int32)[:, None]
    scalar_init = jnp.dot(embed_table, onehot.astype(jnp.bfloat16), preferred_element_type=jnp.float32)
    node_state = jnp.concatenate([scalar_init[None], jnp.zeros((8, C, ATOMS), jnp.float32)], axis=0)
    offsets = (jnp.arange(slab_total, dtype=jnp.int32) * A_DEV)[:, None]
    inner_source = inner_edges[0].reshape(slab_total, E_IN) + offsets
    inner_target = inner_edges[1].reshape(slab_total, E_IN)
    halo_before = jnp.roll(halo_index, 1, axis=0)[:, 1, :] + jnp.roll(offsets, 1, axis=0)
    halo_after = jnp.roll(halo_index, -1, axis=0)[:, 0, :] + jnp.roll(offsets, -1, axis=0)
    halo_atoms = jnp.concatenate([halo_before, halo_after], axis=1)
    halo_slot = outer_edges[0].reshape(slab_total, E_OUT)
    outer_source = jnp.take_along_axis(halo_atoms, halo_slot, axis=1)
    outer_target = outer_edges[1].reshape(slab_total, E_OUT)
    sources = jnp.concatenate([inner_source, outer_source], axis=1).astype(jnp.int32)
    targets = jnp.concatenate([inner_target, outer_target], axis=1).astype(jnp.int32)
    vectors = jnp.concatenate([inner_vec.reshape(3, slab_total, E_IN), outer_vec.reshape(3, slab_total, E_OUT)], axis=2)
    vectors = jnp.transpose(vectors, (1, 0, 2))
    inner_live = (jnp.arange(E_IN, dtype=jnp.int32)[None, :] < edge_count[:, 0:1]).astype(jnp.float32)
    outer_live = (jnp.arange(E_OUT, dtype=jnp.int32)[None, :] < edge_count[:, 1:2]).astype(jnp.float32)
    live_mask = jnp.concatenate([inner_live, outer_live], axis=1)
    for layer_index in range(LAYERS):
        rounded = node_state.astype(jnp.bfloat16)
        features = mix_channels(mix_in[layer_index], rounded).astype(jnp.bfloat16)
        layer_weights = (radial_in[layer_index], radial_mid[layer_index], radial_out[layer_index])

        def per_slab(carried, pieces):
            slab_sources, slab_targets, slab_vectors, slab_live = pieces
            source = jnp.take(features, slab_sources, axis=2)
            directions, bessel = geometry(slab_vectors, NB)
            message = edge_messages(source, directions, bessel, slab_live, layer_weights)
            summed = jnp.zeros((9, C, A_DEV), jnp.float32).at[:, :, slab_targets].add(message)
            return (carried, summed)
        _, slab_sums = lax.scan(per_slab, jnp.zeros((), jnp.float32), (sources, targets, vectors, live_mask))
        aggregated = jnp.transpose(slab_sums, (1, 2, 0, 3)).reshape(9, C, ATOMS)
        aggregated = (aggregated * neighbour_norm).astype(jnp.bfloat16)
        node_state = node_state + gate_update(aggregated, mix_scalar[layer_index], mix_irrep[layer_index])
    readout_part = lax.optimization_barrier(jnp.sum(node_state[0] * readout[:, None], axis=0))
    species_part = lax.optimization_barrier(jnp.sum(onehot.astype(jnp.float32) * species_energy[:, None], axis=0))
    live_atoms = (jnp.arange(ATOMS, dtype=jnp.int32) % A_DEV < jnp.repeat(atom_count, A_DEV)).astype(jnp.float32)
    atom_energy = (readout_part + species_part) * live_atoms
    mean_energy = jnp.sum(atom_energy) / ATOMS
    return (node_state, atom_energy, mean_energy)
```

```python
import functools
import math

import jax
import jax.numpy as jnp
from jax import lax
from jax.sharding import Mesh
from jax.experimental import pallas as pl
from jax.experimental.pallas import tpu as pltpu
from jax.sharding import PartitionSpec as P

SLAB = ("slab_0", "slab_1", "slab_2", "slab_3")


cutoff = 5.0
neighbour_norm = 1.0 / math.sqrt(48.0)
half_root = 0.5 * math.sqrt(3.0)


def passed_along(array, axis, by):
    devices = lax.axis_size(axis)
    return lax.ppermute(array, axis, [(i, (i + by) % devices) for i in range(devices)])


def one_axis_at_a_time(array, axes):
    return functools.reduce(lax.psum, axes, array)


def mix_channels(weights, rounded):
    scalar_part = jnp.dot(weights[0], rounded[0], preferred_element_type=jnp.float32)[None]
    vector_part = jnp.einsum(
        "oi,kia->koa", weights[1], rounded[1:4], preferred_element_type=jnp.float32
    )
    tensor_part = jnp.einsum(
        "oi,kia->koa", weights[2], rounded[4:9], preferred_element_type=jnp.float32
    )
    return jnp.concatenate([scalar_part, vector_part, tensor_part], axis=0)


def gate_update(aggregated, scalar_weight, irrep_weight):
    channels = aggregated.shape[1]
    mixed_scalar = jnp.dot(scalar_weight, aggregated[0], preferred_element_type=jnp.float32)
    mixed_vector = jnp.einsum(
        "oi,kia->koa", irrep_weight[0], aggregated[1:4], preferred_element_type=jnp.float32
    )
    mixed_tensor = jnp.einsum(
        "oi,kia->koa", irrep_weight[1], aggregated[4:9], preferred_element_type=jnp.float32
    )
    new_scalar = jax.nn.silu(mixed_scalar[:channels])[None]
    new_vector = jax.nn.sigmoid(mixed_scalar[channels : 2 * channels])[None] * mixed_vector
    new_tensor = jax.nn.sigmoid(mixed_scalar[2 * channels :])[None] * mixed_tensor
    return jnp.concatenate([new_scalar, new_vector, new_tensor], axis=0)


def sine_of_pi_times(turns):
    nearest = jnp.round(turns)
    rest = turns - nearest
    half = 0.5 * nearest
    sign = 1.0 - 4.0 * (half - jnp.floor(half))
    square = rest * rest
    series = jnp.float32(-0.0073704309)
    series = series * square + 0.08214588661112823
    series = series * square - 0.5992645293207921
    series = series * square + 2.550164039877345
    series = series * square - 5.16771278004997
    series = series * square + 3.141592653589793
    return series * (rest * sign)


def silu_of_twice(half):
    return half + half * jnp.tanh(half)


def edge_kernel(
    count_ref,
    table_ref,
    edges_ref,
    vec_ref,
    radial_in_ref,
    radial_mid_ref,
    radial_out_ref,
    *rest,
    column,
    block,
    channels,
    last,
):
    if last:
        before_ref, out_ref, weight_sc, source_sc, message_sc, unit_sc, sum_sc = rest
    else:
        out_ref, weight_sc, source_sc, message_sc, unit_sc, sum_sc = rest
    count = count_ref[0, column]
    atoms = table_ref.shape[1]
    rows = table_ref.shape[0]
    sum_sc[...] = jnp.zeros_like(sum_sc)
    slots = lax.broadcasted_iota(jnp.int32, (atoms, 1), 0).astype(jnp.float32).astype(jnp.bfloat16)
    orders = (lax.broadcasted_iota(jnp.int32, (8, 1), 0) + 1).astype(jnp.float32)
    one = jnp.ones((), jnp.bfloat16)
    zero = jnp.zeros((), jnp.bfloat16)

    def visit(index, carry):
        offset = pl.multiple_of(index * block, block)
        vec = vec_ref[:, pl.ds(offset, block)]
        x, y, z = vec[0:1], vec[1:2], vec[2:3]
        squared = x * x + y * y + z * z
        length = jnp.sqrt(squared)
        inverse = lax.rsqrt(squared + 0.25)
        fraction = jnp.minimum(length * (1.0 / cutoff), 1.0)
        cubed = fraction * fraction * fraction
        envelope = 1.0 + cubed * cubed * (-28.0 + fraction * (48.0 - 21.0 * fraction))
        height = math.sqrt(2.0 / cutoff) * inverse * envelope
        bessel = sine_of_pi_times(orders * (length * (1.0 / cutoff))) * height
        unit_sc[0:1, :] = x * inverse
        unit_sc[1:2, :] = y * inverse
        unit_sc[2:3, :] = z * inverse
        hidden = silu_of_twice(
            jnp.dot(
                radial_in_ref[...], bessel.astype(jnp.bfloat16), preferred_element_type=jnp.float32
            )
        ).astype(jnp.bfloat16)
        hidden = silu_of_twice(
            jnp.dot(radial_mid_ref[...], hidden, preferred_element_type=jnp.float32)
        ).astype(jnp.bfloat16)
        weight_sc[...] = jnp.dot(radial_out_ref[...], hidden, preferred_element_type=jnp.float32)
        pair = edges_ref[:, pl.ds(offset, block)]
        source = pair[0:1].astype(jnp.float32).astype(jnp.bfloat16)
        source_onehot = jnp.where(slots == source, one, zero)
        source_sc[...] = jnp.dot(
            table_ref[...], source_onehot, preferred_element_type=jnp.float32
        )
        for lane in range(0, block, 128):
            span = slice(lane, lane + 128)
            x, y, z = (jnp.broadcast_to(unit_sc[k : k + 1, span], (16, 128)) for k in range(3))
            hx, hy, hz = half_root * x, half_root * y, half_root * z
            for group in range(0, channels, 16):

                def feature(k):
                    return source_sc[k * channels + group : k * channels + group + 16, span]

                def weight(p):
                    return weight_sc[p * channels + group : p * channels + group + 16, span]

                def put(k, value):
                    upper = value.astype(jnp.bfloat16)
                    lower = (value - upper.astype(jnp.float32)).astype(jnp.bfloat16)
                    row = k * channels + group
                    message_sc[row : row + 16, span] = upper
                    message_sc[rows + row : rows + row + 16, span] = lower

                t1, t2, t3, t4, t5 = (feature(k) for k in range(4, 9))
                v1, v2, v3 = (feature(k) for k in range(1, 4))
                s = feature(0)
                t5_part, t3_part = half_root * t5, 0.5 * t3
                g1 = hy * t1 + hz * t4 + x * (t5_part - t3_part)
                g2 = hx * t1 + hz * t2 - y * (t5_part + t3_part)
                g3 = hy * t2 + hx * t4 + z * t3
                put(
                    0,
                    weight(0) * s
                    + weight(1) * (x * g1 + y * g2 + z * g3)
                    + weight(2) * (x * v1 + y * v2 + z * v3),
                )
                a = weight(3) * s
                w4, w5, w6 = weight(4), weight(5), weight(6)
                p1, p2, p3 = w5 * v1, w5 * v2, w5 * v3
                put(1, a * x + w4 * v1 + (p2 * z - p3 * y) + w6 * g1)
                put(2, a * y + w4 * v2 + (p3 * x - p1 * z) + w6 * g2)
                put(3, a * z + w4 * v3 + (p1 * y - p2 * x) + w6 * g3)
                a = weight(7) * s
                w8, w9 = weight(8), weight(9)
                p1, p2, p3 = w9 * v1 + a * x, w9 * v2 + a * y, w9 * v3 + a * z
                put(4, w8 * t1 + (hy * p1 + hx * p2))
                put(5, w8 * t2 + (hz * p2 + hy * p3))
                put(6, w8 * t3 + (z * p3 - 0.5 * (x * p1 + y * p2)))
                put(7, w8 * t4 + (hz * p1 + hx * p3))
                put(8, w8 * t5 + (hx * p1 - hy * p2))
        place = lax.broadcasted_iota(jnp.int32, (1, block), 1) + offset
        target = jnp.where(place < count, pair[1:2], -1).astype(jnp.float32).astype(jnp.bfloat16)
        target_onehot = jnp.where(slots == target, one, zero)
        sum_sc[...] += lax.dot_general(
            message_sc[...],
            target_onehot,
            (((1,), (1,)), ((), ())),
            preferred_element_type=jnp.float32,
        )
        return carry

    lax.fori_loop(0, (count + block - 1) // block, visit, 0)
    total = sum_sc[0:rows, :] + sum_sc[rows : 2 * rows, :]
    if last:
        total = (total + before_ref[...]) * neighbour_norm
    out_ref[...] = total.astype(out_ref.dtype)


def sum_edges(edge_count, table, edges, vec, layer_weights, column, before=None):
    radial_in, radial_mid, radial_out = layer_weights
    rows, atoms = table.shape
    block = min(1024, edges.shape[1])
    paths = radial_out.shape[0]
    in_vmem = pl.BlockSpec(memory_space=pltpu.VMEM)
    last = before is not None
    arrays = [edge_count, table, edges, vec, radial_in, radial_mid, radial_out]
    if last:
        arrays.append(before)
    slots = edges.shape[1]
    return pl.pallas_call(
        functools.partial(
            edge_kernel, column=column, block=block, channels=rows // 9, last=last
        ),
        out_shape=jax.ShapeDtypeStruct((rows, atoms), jnp.bfloat16 if last else jnp.float32),
        in_specs=[pl.BlockSpec(memory_space=pltpu.SMEM)] + [in_vmem] * (len(arrays) - 1),
        out_specs=in_vmem,
        scratch_shapes=[
            pltpu.VMEM((paths, block), jnp.float32),
            pltpu.VMEM((rows, block), jnp.float32),
            pltpu.VMEM((2 * rows, block), jnp.bfloat16),
            pltpu.VMEM((8, block), jnp.float32),
            pltpu.VMEM((2 * rows, atoms), jnp.float32),
        ],
        compiler_params=pltpu.CompilerParams(vmem_limit_bytes=40 * 2**20),
        cost_estimate=pl.CostEstimate(
            flops=slots * 400000, bytes_accessed=slots * 24, transcendentals=0
        ),
    )(*arrays)


def local(
    species,
    atom_count,
    halo_index,
    edge_count,
    inner_edges,
    outer_edges,
    inner_vec,
    outer_vec,
    embed_table,
    radial_in,
    radial_mid,
    radial_out,
    mix_in,
    mix_scalar,
    mix_irrep,
    readout,
    species_energy,
):
    atom_total = species.shape[0]
    species_total = embed_table.shape[1]
    onehot = species[None, :] == jnp.arange(species_total, dtype=jnp.int32)[:, None]
    scalar_init = jnp.dot(
        embed_table, onehot.astype(jnp.bfloat16), preferred_element_type=jnp.float32
    )
    node_state = jnp.concatenate(
        [scalar_init[None], jnp.zeros((8,) + scalar_init.shape, jnp.float32)], axis=0
    )
    channels = mix_in.shape[2]
    atom_slots = jnp.arange(atom_total, dtype=jnp.int32)
    to_left, to_right = (
        (atom_slots[:, None] == halo_index[0, side][None, :]).astype(jnp.bfloat16)
        for side in (0, 1)
    )
    first = lax.axis_index("chan") == 0
    for layer_index in range(radial_in.shape[0]):
        rounded = node_state.astype(jnp.bfloat16)
        features = mix_channels(mix_in[layer_index], rounded).astype(jnp.bfloat16)
        table = features.reshape(9 * channels, atom_total)
        layer_weights = (
            radial_in[layer_index] * 0.5,
            radial_mid[layer_index] * 0.5,
            radial_out[layer_index].reshape(-1, radial_out.shape[3]),
        )

        def boundary(choice):
            return jnp.dot(table, choice, preferred_element_type=jnp.float32).astype(jnp.bfloat16)

        from_left = passed_along(boundary(to_right), SLAB, 1)
        from_right = passed_along(boundary(to_left), SLAB, -1)
        summed = sum_edges(edge_count, table, inner_edges, inner_vec, layer_weights, 0)
        halo_table = jnp.concatenate([from_left, from_right], axis=1)
        aggregated = sum_edges(
            edge_count, halo_table, outer_edges, outer_vec, layer_weights, 1, summed
        ).reshape(9, channels, atom_total)
        other = lax.ppermute(aggregated, "chan", [(0, 1), (1, 0)])
        all_channels = jnp.concatenate(
            [jnp.where(first, aggregated, other), jnp.where(first, other, aggregated)], axis=1
        )
        node_state = node_state + gate_update(
            all_channels, mix_scalar[layer_index], mix_irrep[layer_index]
        )
    readout_part = jnp.sum(node_state[0] * readout[:, None], axis=0)
    species_part = jnp.sum(onehot.astype(jnp.float32) * species_energy[:, None], axis=0)
    live_atoms = (jnp.arange(atom_total, dtype=jnp.int32) < atom_count[0]).astype(jnp.float32)
    atom_energy = (readout_part + species_part) * live_atoms
    energy_sum = one_axis_at_a_time(jnp.sum(atom_energy), SLAB)
    mean_energy = energy_sum / (atom_total * lax.axis_size(SLAB))
    return (node_state, atom_energy, mean_energy)


def solution(mesh):
    finer = Mesh(
        mesh.devices.reshape(8, 2, 4, 2, mesh.shape["chan"]),
        ("slab_0", "slab_1", "slab_2", "slab_3", "chan"),
    )
    placed = (
        P(SLAB),
        P(SLAB),
        P(SLAB, None, None),
        P(SLAB, None),
        P(None, SLAB),
        P(None, SLAB),
        P(None, SLAB),
        P(None, SLAB),
        P(),
        P(),
        P(),
        P(None, None, "chan", None),
        P(None, None, "chan", None),
        P(),
        P(),
        P(),
        P(),
    )
    return jax.shard_map(
        local,
        mesh=finer,
        in_specs=placed,
        out_specs=(P(None, None, SLAB), P(SLAB), P()),
        check_vma=False,
    )
```

```python
import functools
import math

import jax
import jax.numpy as jnp
from jax import lax
from jax.sharding import Mesh
from jax.experimental import pallas as pl
from jax.experimental.pallas import tpu as pltpu
from jax.sharding import PartitionSpec as P

SLAB = ("slab_0", "slab_1", "slab_2", "slab_3")


cutoff = 5.0
neighbour_norm = 1.0 / math.sqrt(48.0)
half_root = 0.5 * math.sqrt(3.0)


def passed_along(array, axis, by):
    devices = lax.axis_size(axis)
    return lax.ppermute(array, axis, [(i, (i + by) % devices) for i in range(devices)])


def mix_channels(weights, rounded):
    scalar_part = jnp.dot(weights[0], rounded[0], preferred_element_type=jnp.float32)[None]
    vector_part = jnp.einsum(
        "oi,kia->koa", weights[1], rounded[1:4], preferred_element_type=jnp.float32
    )
    tensor_part = jnp.einsum(
        "oi,kia->koa", weights[2], rounded[4:9], preferred_element_type=jnp.float32
    )
    return jnp.concatenate([scalar_part, vector_part, tensor_part], axis=0)


def gate_update(aggregated, scalar_weight, irrep_weight):
    channels = aggregated.shape[1]
    mixed_scalar = jnp.dot(scalar_weight, aggregated[0], preferred_element_type=jnp.float32)
    mixed_vector = jnp.einsum(
        "oi,kia->koa", irrep_weight[0], aggregated[1:4], preferred_element_type=jnp.float32
    )
    mixed_tensor = jnp.einsum(
        "oi,kia->koa", irrep_weight[1], aggregated[4:9], preferred_element_type=jnp.float32
    )
    new_scalar = jax.nn.silu(mixed_scalar[:channels])[None]
    new_vector = jax.nn.sigmoid(mixed_scalar[channels : 2 * channels])[None] * mixed_vector
    new_tensor = jax.nn.sigmoid(mixed_scalar[2 * channels :])[None] * mixed_tensor
    return jnp.concatenate([new_scalar, new_vector, new_tensor], axis=0)


def sine_of_pi_times(turns):
    nearest = jnp.round(turns)
    rest = turns - nearest
    half = 0.5 * nearest
    sign = 1.0 - 4.0 * (half - jnp.floor(half))
    square = rest * rest
    series = jnp.float32(-0.0073704309)
    series = series * square + 0.08214588661112823
    series = series * square - 0.5992645293207921
    series = series * square + 2.550164039877345
    series = series * square - 5.16771278004997
    series = series * square + 3.141592653589793
    return series * (rest * sign)


def silu_of_twice(half):
    return half + half * jnp.tanh(half)


def radial_kernel(count_ref, vec_ref, first_ref, middle_ref, hidden_ref, unit_ref, *, column, block):
    orders = (lax.broadcasted_iota(jnp.int32, (8, 1), 0) + 1).astype(jnp.float32)

    def visit(index, carry):
        span = pl.ds(pl.multiple_of(index * block, block), block)
        vec = vec_ref[:, span]
        x, y, z = vec[0:1], vec[1:2], vec[2:3]
        squared = x * x + y * y + z * z
        length = jnp.sqrt(squared)
        inverse = lax.rsqrt(squared + 0.25)
        fraction = jnp.minimum(length * (1.0 / cutoff), 1.0)
        cubed = fraction * fraction * fraction
        envelope = 1.0 + cubed * cubed * (-28.0 + fraction * (48.0 - 21.0 * fraction))
        height = math.sqrt(2.0 / cutoff) * inverse * envelope
        bessel = sine_of_pi_times(orders * (length * (1.0 / cutoff))) * height
        unit_ref[0:1, span] = x * inverse
        unit_ref[1:2, span] = y * inverse
        unit_ref[2:3, span] = z * inverse
        hidden = silu_of_twice(
            jnp.dot(first_ref[...], bessel.astype(jnp.bfloat16), preferred_element_type=jnp.float32)
        ).astype(jnp.bfloat16)
        hidden_ref[:, span] = silu_of_twice(
            jnp.dot(middle_ref[...], hidden, preferred_element_type=jnp.float32)
        ).astype(jnp.bfloat16)
        return carry

    lax.fori_loop(0, (count_ref[0, column] + block - 1) // block, visit, 0)


def radial_net(edge_count, vec, first, middle, column):
    slots = vec.shape[1]
    in_vmem = pl.BlockSpec(memory_space=pltpu.VMEM)
    return pl.pallas_call(
        functools.partial(radial_kernel, column=column, block=min(2048, slots)),
        out_shape=(
            jax.ShapeDtypeStruct((middle.shape[0], slots), jnp.bfloat16),
            jax.ShapeDtypeStruct((8, slots), jnp.float32),
        ),
        in_specs=[pl.BlockSpec(memory_space=pltpu.SMEM)] + [in_vmem] * 3,
        out_specs=(in_vmem, in_vmem),
        compiler_params=pltpu.CompilerParams(vmem_limit_bytes=40 * 2**20),
        cost_estimate=pl.CostEstimate(
            flops=slots * 40000, bytes_accessed=slots * 300, transcendentals=0
        ),
    )(edge_count, vec, first, middle)


def edge_kernel(
    count_ref,
    table_ref,
    edges_ref,
    hidden_ref,
    unit_ref,
    mix_ref,
    *rest,
    column,
    block,
    channels,
    first_row,
    last,
):
    if last:
        before_ref, out_ref, *scratch = rest
    else:
        out_ref, *scratch = rest
    weight_sc, source_sc, message_sc, direction_sc = (scratch[2 * k : 2 * k + 2] for k in range(4))
    target_sc, sum_sc = scratch[8:]
    count = count_ref[0, column]
    blocks = (count + block - 1) // block
    slots = edges_ref.shape[1]
    rows, atoms = table_ref.shape
    breadth = mix_ref.shape[1]
    sum_sc[...] = jnp.zeros_like(sum_sc)
    message_sc[1][...] = jnp.zeros_like(message_sc[1])
    names = lax.broadcasted_iota(jnp.int32, (atoms, 1), 0).astype(jnp.float32).astype(jnp.bfloat16)
    one = jnp.ones((), jnp.bfloat16)
    zero = jnp.zeros((), jnp.bfloat16)

    def span_of(index):
        start = jnp.clip(index * block, 0, slots - block)
        return pl.ds(pl.multiple_of(start, block), block)

    def expansion(index, into):
        span = span_of(index)
        source = edges_ref[0:1, span].astype(jnp.float32).astype(jnp.bfloat16)
        hidden = hidden_ref[first_row : first_row + breadth, span]
        direction_sc[into][0:3, :] = unit_ref[0:3, span]

        def gather(lane):
            cut = slice(lane, lane + 256)
            onehot = jnp.where(names == source[:, cut], one, zero)
            source_sc[into][:, cut] = jnp.dot(
                table_ref[...], onehot, preferred_element_type=jnp.float32
            )

        def weigh(lane):
            cut = slice(lane, lane + 256)
            weight_sc[into][:, cut] = jnp.dot(
                mix_ref[...], hidden[:, cut], preferred_element_type=jnp.float32
            )

        lanes = range(0, block, 256)
        return [functools.partial(gather, k) for k in lanes] + [
            functools.partial(weigh, k) for k in lanes
        ]

    def reduction(index, held):
        place = lax.broadcasted_iota(jnp.int32, (1, block), 1) + index * block
        target = jnp.where(place < count, edges_ref[1:2, span_of(index)], -1)
        target = target.astype(jnp.float32).astype(jnp.bfloat16)
        for lane in range(0, block, 256):
            cut = slice(lane, lane + 256)
            target_sc[:, cut] = jnp.where(names == target[:, cut], one, zero)

        def scatter(row):
            cut = slice(row, row + rows)
            sum_sc[cut, :] += lax.dot_general(
                message_sc[held][cut, :],
                target_sc[...],
                (((1,), (1,)), ((), ())),
                preferred_element_type=jnp.float32,
            )

        return [functools.partial(scatter, 0), functools.partial(scatter, rows)]

    def messages(held, lane, group):
        span = slice(lane, lane + 256)
        x, y, z = (
            jnp.broadcast_to(direction_sc[held][k : k + 1, span], (8, 256)) for k in range(3)
        )
        hx, hy, hz = half_root * x, half_root * y, half_root * z

        def feature(k):
            return source_sc[held][k * channels + group : k * channels + group + 8, span]

        def weight(p):
            return weight_sc[held][p * channels + group : p * channels + group + 8, span]

        def put(k, value):
            upper = value.astype(jnp.bfloat16)
            lower = (value - upper.astype(jnp.float32)).astype(jnp.bfloat16)
            row = k * channels + group
            message_sc[held][row : row + 8, span] = upper
            message_sc[held][rows + row : rows + row + 8, span] = lower

        t1, t2, t3, t4, t5 = (feature(k) for k in range(4, 9))
        t5_part, t3_part = half_root * t5, 0.5 * t3
        g1 = hy * t1 + hz * t4 + x * (t5_part - t3_part)
        g2 = hx * t1 + hz * t2 - y * (t5_part + t3_part)
        g3 = hy * t2 + hx * t4 + z * t3
        v1, v2, v3 = (feature(k) for k in range(1, 4))
        s = feature(0)
        put(
            0,
            weight(0) * s
            + weight(1) * (x * g1 + y * g2 + z * g3)
            + weight(2) * (x * v1 + y * v2 + z * v3),
        )
        a = weight(3) * s
        w4, w5, w6 = weight(4), weight(5), weight(6)
        p1, p2, p3 = w5 * v1, w5 * v2, w5 * v3
        put(1, a * x + w4 * v1 + (p2 * z - p3 * y) + w6 * g1)
        put(2, a * y + w4 * v2 + (p3 * x - p1 * z) + w6 * g2)
        put(3, a * z + w4 * v3 + (p1 * y - p2 * x) + w6 * g3)
        a = weight(7) * s
        w8, w9 = weight(8), weight(9)
        p1, p2, p3 = w9 * v1 + a * x, w9 * v2 + a * y, w9 * v3 + a * z
        put(4, w8 * t1 + (hy * p1 + hx * p2))
        put(5, w8 * t2 + (hz * p2 + hy * p3))
        put(6, w8 * t3 + (z * p3 - 0.5 * (x * p1 + y * p2)))
        put(7, w8 * t4 + (hz * p1 + hx * p3))
        put(8, w8 * t5 + (hx * p1 - hy * p2))

    def stage(index, held):
        pieces = expansion(index + 1, 1 - held) + reduction(index - 1, 1 - held)
        units = [(lane, group) for lane in range(0, block, 256) for group in range(0, channels, 8)]
        done = 0
        for position, unit in enumerate(units):
            while done < len(pieces) and done * len(units) * 4 < (position + 1) * len(pieces) * 5:
                pieces[done]()
                done += 1
            messages(held, *unit)

    def drain(held):
        for piece in reduction(blocks - 1, held):
            piece()

    for piece in expansion(0, 0):
        piece()

    def visit(index, carry):
        pl.when(2 * index < blocks)(lambda: stage(2 * index, 0))
        pl.when(2 * index + 1 < blocks)(lambda: stage(2 * index + 1, 1))
        return carry

    lax.fori_loop(0, (blocks + 1) // 2, visit, 0)
    odd = lax.rem(blocks, 2)
    pl.when(odd == 1)(lambda: drain(0))
    pl.when(odd == 0)(lambda: drain(1))
    total = sum_sc[0:rows, :] + sum_sc[rows : 2 * rows, :]
    if last:
        total = (total + before_ref[...]) * neighbour_norm
    out_ref[...] = total.astype(out_ref.dtype)


def sum_edges(edge_count, table, edges, hidden, unit, mix, layer_index, column, before=None):
    rows, atoms = table.shape
    slots = edges.shape[1]
    last = before is not None
    block = min(512 if last else 1024, slots)
    paths, breadth = mix.shape
    in_vmem = pl.BlockSpec(memory_space=pltpu.VMEM)
    arrays = [edge_count, table, edges, hidden, unit, mix]
    if last:
        arrays.append(before)

    def two(shape, dtype):
        return [pltpu.VMEM(shape, dtype)] * 2

    return pl.pallas_call(
        functools.partial(
            edge_kernel,
            column=column,
            block=block,
            channels=rows // 9,
            first_row=layer_index * breadth,
            last=last,
        ),
        out_shape=jax.ShapeDtypeStruct((rows, atoms), jnp.bfloat16 if last else jnp.float32),
        in_specs=[pl.BlockSpec(memory_space=pltpu.SMEM)] + [in_vmem] * (len(arrays) - 1),
        out_specs=in_vmem,
        scratch_shapes=two((paths, block), jnp.float32)
        + two((rows, block), jnp.float32)
        + two((2 * rows, block), jnp.bfloat16)
        + two((8, block), jnp.float32)
        + [pltpu.VMEM((atoms, block), jnp.bfloat16), pltpu.VMEM((2 * rows, atoms), jnp.float32)],
        compiler_params=pltpu.CompilerParams(vmem_limit_bytes=40 * 2**20),
        cost_estimate=pl.CostEstimate(
            flops=slots * 400000, bytes_accessed=slots * 300, transcendentals=0
        ),
    )(*arrays)


def total_kernel(part_ref, total_ref, near_sc, far_sc, near_send, near_recv, far_send, far_recv):
    far, *near = SLAB
    sizes = [lax.axis_size(name) for name in near]
    place = [lax.axis_index(name) for name in near]
    far_size = lax.axis_size(far)
    far_place = lax.axis_index(far)
    near_total = math.prod(sizes)

    def split(step):
        return step // (sizes[1] * sizes[2]), step // sizes[2] % sizes[1], step % sizes[2]

    def near_device(step):
        return {
            name: (at + by) % size for name, at, by, size in zip(near, place, split(step), sizes)
        }

    def near_sender(step):
        at = [(p + size - by) % size for p, by, size in zip(place, split(step), sizes)]
        return (at[0] * sizes[1] + at[1]) * sizes[2] + at[2]

    def near_copy(step, slot):
        return pltpu.make_async_remote_copy(
            src_ref=part_ref,
            dst_ref=near_sc.at[slot],
            send_sem=near_send.at[step],
            recv_sem=near_recv.at[slot],
            device_id=near_device(step),
            device_id_type=pl.DeviceIdType.MESH,
        )

    def far_copy(step, slot):
        return pltpu.make_async_remote_copy(
            src_ref=near_sc,
            dst_ref=far_sc.at[slot],
            send_sem=far_send.at[step],
            recv_sem=far_recv.at[slot],
            device_id={far: (far_place + step) % far_size},
            device_id_type=pl.DeviceIdType.MESH,
        )

    barrier = pltpu.get_barrier_semaphore()
    for step in range(1, near_total):
        pl.semaphore_signal(
            barrier, inc=1, device_id=near_device(step), device_id_type=pl.DeviceIdType.MESH
        )
    for step in range(1, far_size):
        pl.semaphore_signal(
            barrier,
            inc=1,
            device_id={far: (far_place + step) % far_size},
            device_id_type=pl.DeviceIdType.MESH,
        )
    pl.semaphore_wait(barrier, near_total + far_size - 2)
    mine = near_sender(0)
    near_sc[mine] = part_ref[...]
    for step in range(1, near_total):
        near_copy(step, mine).start()
    for step in range(1, near_total):
        near_copy(step, near_sender(step)).wait_recv()
    for step in range(1, far_size):
        far_copy(step, far_place).start()
    far_sc[far_place] = near_sc[...]
    for step in range(1, far_size):
        far_copy(step, (far_place + far_size - step) % far_size).wait_recv()
    total_ref[...] = jnp.sum(far_sc[...], axis=(0, 1))
    for step in range(1, near_total):
        near_copy(step, mine).wait_send()
    for step in range(1, far_size):
        far_copy(step, far_place).wait_send()


def total_over_slabs(part):
    lanes = part.shape[1]
    far_size, near_total = lax.axis_size(SLAB[0]), lax.axis_size(SLAB[1:])
    return pl.pallas_call(
        total_kernel,
        out_shape=jax.ShapeDtypeStruct((1, lanes), jnp.float32),
        in_specs=[pl.BlockSpec(memory_space=pltpu.VMEM)],
        out_specs=pl.BlockSpec(memory_space=pltpu.VMEM),
        scratch_shapes=[
            pltpu.VMEM((near_total, 1, lanes), jnp.float32),
            pltpu.VMEM((far_size, near_total, 1, lanes), jnp.float32),
            pltpu.SemaphoreType.DMA((near_total,)),
            pltpu.SemaphoreType.DMA((near_total,)),
            pltpu.SemaphoreType.DMA((far_size,)),
            pltpu.SemaphoreType.DMA((far_size,)),
        ],
        compiler_params=pltpu.CompilerParams(collective_id=0, has_side_effects=True),
    )(part)


def local(
    species,
    atom_count,
    halo_index,
    edge_count,
    inner_edges,
    outer_edges,
    inner_vec,
    outer_vec,
    embed_table,
    radial_in,
    radial_mid,
    radial_out,
    mix_in,
    mix_scalar,
    mix_irrep,
    readout,
    species_energy,
):
    atom_total = species.shape[0]
    species_total = embed_table.shape[1]
    onehot = species[None, :] == jnp.arange(species_total, dtype=jnp.int32)[:, None]
    scalar_init = jnp.dot(
        embed_table, onehot.astype(jnp.bfloat16), preferred_element_type=jnp.float32
    )
    node_state = jnp.concatenate(
        [scalar_init[None], jnp.zeros((8,) + scalar_init.shape, jnp.float32)], axis=0
    )
    channels = mix_in.shape[2]
    atom_slots = jnp.arange(atom_total, dtype=jnp.int32)
    to_left, to_right = (
        (atom_slots[:, None] == halo_index[0, side][None, :]).astype(jnp.bfloat16)
        for side in (0, 1)
    )
    first = lax.axis_index("chan") == 0
    layers, breadth, _ = radial_in.shape
    first_weights = (radial_in * 0.5).reshape(layers * breadth, -1)
    middle_weights = jnp.zeros((layers * breadth, layers * breadth), jnp.bfloat16)
    for layer_index in range(layers):
        cut = slice(layer_index * breadth, (layer_index + 1) * breadth)
        middle_weights = middle_weights.at[cut, cut].set(radial_mid[layer_index] * 0.5)
    for layer_index in range(layers):
        rounded = node_state.astype(jnp.bfloat16)
        features = mix_channels(mix_in[layer_index], rounded).astype(jnp.bfloat16)
        table = features.reshape(9 * channels, atom_total)
        mix = radial_out[layer_index].reshape(-1, breadth)

        def boundary(choice):
            return jnp.dot(table, choice, preferred_element_type=jnp.float32).astype(jnp.bfloat16)

        from_left = passed_along(boundary(to_right), SLAB, 1)
        from_right = passed_along(boundary(to_left), SLAB, -1)
        if layer_index == 0:
            inner_net = radial_net(edge_count, inner_vec, first_weights, middle_weights, 0)
            outer_net = radial_net(edge_count, outer_vec, first_weights, middle_weights, 1)
        summed = sum_edges(edge_count, table, inner_edges, *inner_net, mix, layer_index, 0)
        halo_table = jnp.concatenate([from_left, from_right], axis=1)
        aggregated = sum_edges(
            edge_count, halo_table, outer_edges, *outer_net, mix, layer_index, 1, summed
        ).reshape(9, channels, atom_total)
        other = lax.ppermute(aggregated, "chan", [(0, 1), (1, 0)])
        all_channels = jnp.concatenate(
            [jnp.where(first, aggregated, other), jnp.where(first, other, aggregated)], axis=1
        )
        node_state = node_state + gate_update(
            all_channels, mix_scalar[layer_index], mix_irrep[layer_index]
        )
    readout_part = jnp.sum(node_state[0] * readout[:, None], axis=0)
    species_part = jnp.sum(onehot.astype(jnp.float32) * species_energy[:, None], axis=0)
    live_atoms = (jnp.arange(atom_total, dtype=jnp.int32) < atom_count[0]).astype(jnp.float32)
    atom_energy = (readout_part + species_part) * live_atoms
    energy_sum = jnp.sum(total_over_slabs(jnp.sum(atom_energy.reshape(-1, 128), axis=0)[None]))
    mean_energy = energy_sum / (atom_total * lax.axis_size(SLAB))
    return (node_state, atom_energy, mean_energy)


def solution(mesh):
    finer = Mesh(
        mesh.devices.reshape(8, 2, 4, 2, mesh.shape["chan"]),
        ("slab_0", "slab_1", "slab_2", "slab_3", "chan"),
    )
    placed = (
        P(SLAB),
        P(SLAB),
        P(SLAB, None, None),
        P(SLAB, None),
        P(None, SLAB),
        P(None, SLAB),
        P(None, SLAB),
        P(None, SLAB),
        P(),
        P(),
        P(),
        P(None, None, "chan", None),
        P(None, None, "chan", None),
        P(),
        P(),
        P(),
        P(),
    )
    return jax.shard_map(
        local,
        mesh=finer,
        in_specs=placed,
        out_specs=(P(None, None, SLAB), P(SLAB), P()),
        check_vma=False,
    )
```

```python
import functools
import math

import jax
import jax.numpy as jnp
from jax import lax
from jax.sharding import Mesh
from jax.experimental import pallas as pl
from jax.experimental.pallas import tpu as pltpu
from jax.sharding import PartitionSpec as P

SLAB = ("slab_0", "slab_1", "slab_2", "slab_3")


cutoff = 5.0
neighbour_norm = 1.0 / math.sqrt(48.0)
half_root = 0.5 * math.sqrt(3.0)


def passed_along(array, axis, by):
    devices = lax.axis_size(axis)
    return lax.ppermute(array, axis, [(i, (i + by) % devices) for i in range(devices)])


def kind_of(component):
    return 0 if component == 0 else 1 if component < 4 else 2


def mix_and_choose(state_ref, mix_ref, halo_ref, layer, table_ref, left_ref, right_ref):
    channels = mix_ref.shape[2]
    atoms = table_ref.shape[1]
    for k in range(9):
        table_ref[k * channels : (k + 1) * channels, :] = jnp.dot(
            mix_ref[layer, kind_of(k)],
            state_ref[k].astype(jnp.bfloat16),
            preferred_element_type=jnp.float32,
        ).astype(jnp.bfloat16)
    for side, out_ref in ((0, left_ref), (1, right_ref)):
        chosen = halo_ref[0, side : side + 1, :]
        names = lax.broadcasted_iota(jnp.int32, (atoms, chosen.shape[1]), 0)
        onehot = jnp.where(names == chosen, 1.0, 0.0).astype(jnp.bfloat16)
        out_ref[...] = jnp.dot(
            table_ref[...], onehot, preferred_element_type=jnp.float32
        ).astype(jnp.bfloat16)


def start_kernel(
    species_ref, embed_ref, mix_ref, halo_ref, state_ref, table_ref, left_ref, right_ref
):
    species = species_ref[...]
    embed = embed_ref[...].astype(jnp.float32)
    scalar = jnp.zeros(state_ref.shape[1:], jnp.float32)
    for kind in range(embed.shape[1]):
        scalar = scalar + jnp.where(species == kind, embed[:, kind : kind + 1], 0.0)
    state_ref[0] = scalar
    state_ref[1:] = jnp.zeros((8, *scalar.shape), jnp.float32)
    mix_and_choose(state_ref, mix_ref, halo_ref, 0, table_ref, left_ref, right_ref)


def update_state(own_ref, other_ref, old_ref, scalar_ref, irrep_ref, new_ref, all_sc, layer):
    channels = own_ref.shape[0] // 9
    wide = old_ref.shape[1]
    me = lax.axis_index("chan")
    for k in range(9):
        for part, ref in ((me, own_ref), (1 - me, other_ref)):
            place = pl.ds(pl.multiple_of(part * channels, channels), channels)
            all_sc[k, place, :] = ref[k * channels : (k + 1) * channels, :]
    mixed = 0.5 * jnp.dot(scalar_ref[layer], all_sc[0], preferred_element_type=jnp.float32)
    new_ref[0] = old_ref[0] + silu_of_twice(mixed[0:wide])
    gates = 0.5 * jnp.tanh(mixed[wide:]) + 0.5
    for k in range(1, 9):
        kind = kind_of(k) - 1
        value = jnp.dot(irrep_ref[layer, kind], all_sc[k], preferred_element_type=jnp.float32)
        new_ref[k] = old_ref[k] + gates[kind * wide : (kind + 1) * wide] * value


def middle_kernel(
    own_ref, other_ref, old_ref, scalar_ref, irrep_ref, mix_ref, halo_ref, *rest, layer
):
    new_ref, table_ref, left_ref, right_ref, all_sc = rest
    update_state(own_ref, other_ref, old_ref, scalar_ref, irrep_ref, new_ref, all_sc, layer)
    mix_and_choose(new_ref, mix_ref, halo_ref, layer + 1, table_ref, left_ref, right_ref)


def final_kernel(
    atom_ref, base_ref, own_ref, other_ref, old_ref, scalar_ref, irrep_ref, *rest, layer
):
    readout_ref, species_ref, new_ref, energy_ref, part_ref, all_sc = rest
    update_state(own_ref, other_ref, old_ref, scalar_ref, irrep_ref, new_ref, all_sc, layer)
    energy = jnp.sum(new_ref[0] * readout_ref[...], axis=0, keepdims=True)
    species = species_ref[...]
    for kind in range(base_ref.shape[0]):
        energy = energy + jnp.where(species == kind, base_ref[kind], 0.0)
    place = lax.broadcasted_iota(jnp.int32, energy.shape, 1)
    energy = jnp.where(place < atom_ref[0], energy, 0.0)
    energy_ref[...] = energy
    part = energy[:, 0:128]
    for lane in range(128, energy.shape[1], 128):
        part = part + energy[:, lane : lane + 128]
    part_ref[...] = part


def node_call(kernel, scalars, arrays, shapes, gathered=None):
    in_vmem = pl.BlockSpec(memory_space=pltpu.VMEM)
    return pl.pallas_call(
        kernel,
        out_shape=tuple(jax.ShapeDtypeStruct(*shape) for shape in shapes),
        in_specs=[pl.BlockSpec(memory_space=pltpu.SMEM)] * len(scalars) + [in_vmem] * len(arrays),
        out_specs=(in_vmem,) * len(shapes),
        scratch_shapes=[] if gathered is None else [pltpu.VMEM(gathered, jnp.bfloat16)],
        compiler_params=pltpu.CompilerParams(vmem_limit_bytes=20 * 2**20),
        cost_estimate=pl.CostEstimate(flops=10**9, bytes_accessed=2 * 10**6, transcendentals=0),
    )(*scalars, *arrays)


def sine_of_pi_times(turns):
    nearest = jnp.round(turns)
    rest = turns - nearest
    half = 0.5 * nearest
    sign = 1.0 - 4.0 * (half - jnp.floor(half))
    square = rest * rest
    series = jnp.float32(-0.0073704309)
    series = series * square + 0.08214588661112823
    series = series * square - 0.5992645293207921
    series = series * square + 2.550164039877345
    series = series * square - 5.16771278004997
    series = series * square + 3.141592653589793
    return series * (rest * sign)


def silu_of_twice(half):
    return half + half * jnp.tanh(half)


def radial_kernel(
    count_ref, inner_ref, outer_ref, first_ref, middle_ref, *outs, block
):
    orders = (lax.broadcasted_iota(jnp.int32, (8, 1), 0) + 1).astype(jnp.float32)
    layers, breadth, _ = first_ref.shape

    def visit_list(column, vec_ref, hidden_ref, unit_ref):
        def visit(index, carry):
            span = pl.ds(pl.multiple_of(index * block, block), block)
            vec = vec_ref[:, span]
            x, y, z = vec[0:1], vec[1:2], vec[2:3]
            squared = x * x + y * y + z * z
            length = jnp.sqrt(squared)
            inverse = lax.rsqrt(squared + 0.25)
            fraction = jnp.minimum(length * (1.0 / cutoff), 1.0)
            cubed = fraction * fraction * fraction
            envelope = 1.0 + cubed * cubed * (-28.0 + fraction * (48.0 - 21.0 * fraction))
            height = math.sqrt(2.0 / cutoff) * inverse * envelope
            bessel = sine_of_pi_times(orders * (length * (1.0 / cutoff))) * height
            bessel = bessel.astype(jnp.bfloat16)
            unit_ref[0:1, span] = x * inverse
            unit_ref[1:2, span] = y * inverse
            unit_ref[2:3, span] = z * inverse
            hidden = [
                silu_of_twice(
                    0.5 * jnp.dot(first_ref[k], bessel, preferred_element_type=jnp.float32)
                ).astype(jnp.bfloat16)
                for k in range(layers)
            ]
            for k in range(layers):
                hidden_ref[k * breadth : (k + 1) * breadth, span] = silu_of_twice(
                    0.5 * jnp.dot(middle_ref[k], hidden[k], preferred_element_type=jnp.float32)
                ).astype(jnp.bfloat16)
            return carry

        lax.fori_loop(0, (count_ref[0, column] + block - 1) // block, visit, 0)

    visit_list(0, inner_ref, *outs[0:2])
    visit_list(1, outer_ref, *outs[2:4])


def radial_net(edge_count, inner_vec, outer_vec, first, middle):
    in_vmem = pl.BlockSpec(memory_space=pltpu.VMEM)
    shapes = []
    for vec in (inner_vec, outer_vec):
        slots = vec.shape[1]
        shapes.append(
            jax.ShapeDtypeStruct((middle.shape[0] * middle.shape[1], slots), jnp.bfloat16)
        )
        shapes.append(jax.ShapeDtypeStruct((8, slots), jnp.float32))
    slots = inner_vec.shape[1] + outer_vec.shape[1]
    return pl.pallas_call(
        functools.partial(radial_kernel, block=min(2048, outer_vec.shape[1])),
        out_shape=tuple(shapes),
        in_specs=[pl.BlockSpec(memory_space=pltpu.SMEM)] + [in_vmem] * 4,
        out_specs=(in_vmem,) * 4,
        compiler_params=pltpu.CompilerParams(vmem_limit_bytes=40 * 2**20),
        cost_estimate=pl.CostEstimate(
            flops=slots * 40000, bytes_accessed=slots * 300, transcendentals=0
        ),
    )(edge_count, inner_vec, outer_vec, first, middle)


def edge_kernel(
    count_ref,
    table_ref,
    edges_ref,
    hidden_ref,
    unit_ref,
    mix_ref,
    *rest,
    column,
    block,
    channels,
    layer,
    last,
):
    if last:
        before_ref, out_ref, *scratch = rest
    else:
        out_ref, *scratch = rest
    weight_sc, source_sc, message_sc, direction_sc = (scratch[2 * k : 2 * k + 2] for k in range(4))
    target_sc, sum_sc = scratch[8:]
    count = count_ref[0, column]
    blocks = (count + block - 1) // block
    slots = edges_ref.shape[1]
    rows, atoms = table_ref.shape
    breadth = mix_ref.shape[3]
    first_row = layer * breadth
    sum_sc[...] = jnp.zeros_like(sum_sc)
    message_sc[1][...] = jnp.zeros_like(message_sc[1])
    names = lax.broadcasted_iota(jnp.int32, (atoms, 1), 0).astype(jnp.float32).astype(jnp.bfloat16)
    one = jnp.ones((), jnp.bfloat16)
    zero = jnp.zeros((), jnp.bfloat16)

    def span_of(index):
        start = jnp.clip(index * block, 0, slots - block)
        return pl.ds(pl.multiple_of(start, block), block)

    def expansion(index, into):
        span = span_of(index)
        source = edges_ref[0:1, span].astype(jnp.float32).astype(jnp.bfloat16)
        hidden = hidden_ref[first_row : first_row + breadth, span]
        direction_sc[into][0:3, :] = unit_ref[0:3, span]

        def gather(lane):
            cut = slice(lane, lane + 256)
            onehot = jnp.where(names == source[:, cut], one, zero)
            source_sc[into][:, cut] = jnp.dot(
                table_ref[...], onehot, preferred_element_type=jnp.float32
            )

        def weigh(lane):
            cut = slice(lane, lane + 256)
            weight_sc[into][:, cut] = jnp.dot(
                mix_ref[layer].reshape(-1, breadth),
                hidden[:, cut],
                preferred_element_type=jnp.float32,
            )

        lanes = range(0, block, 256)
        return [functools.partial(gather, k) for k in lanes] + [
            functools.partial(weigh, k) for k in lanes
        ]

    def reduction(index, held):
        place = lax.broadcasted_iota(jnp.int32, (1, block), 1) + index * block
        target = jnp.where(place < count, edges_ref[1:2, span_of(index)], -1)
        target = target.astype(jnp.float32).astype(jnp.bfloat16)
        for lane in range(0, block, 256):
            cut = slice(lane, lane + 256)
            target_sc[:, cut] = jnp.where(names == target[:, cut], one, zero)

        def scatter(row):
            cut = slice(row, row + rows)
            sum_sc[cut, :] += lax.dot_general(
                message_sc[held][cut, :],
                target_sc[...],
                (((1,), (1,)), ((), ())),
                preferred_element_type=jnp.float32,
            )

        return [functools.partial(scatter, 0), functools.partial(scatter, rows)]

    def messages(held, lane, group):
        span = slice(lane, lane + 256)
        x, y, z = (
            jnp.broadcast_to(direction_sc[held][k : k + 1, span], (8, 256)) for k in range(3)
        )
        hx, hy, hz = half_root * x, half_root * y, half_root * z

        def feature(k):
            return source_sc[held][k * channels + group : k * channels + group + 8, span]

        def weight(p):
            return weight_sc[held][p * channels + group : p * channels + group + 8, span]

        def put(k, value):
            upper = value.astype(jnp.bfloat16)
            lower = (value - upper.astype(jnp.float32)).astype(jnp.bfloat16)
            row = k * channels + group
            message_sc[held][row : row + 8, span] = upper
            message_sc[held][rows + row : rows + row + 8, span] = lower

        t1, t2, t3, t4, t5 = (feature(k) for k in range(4, 9))
        t5_part, t3_part = half_root * t5, 0.5 * t3
        g1 = hy * t1 + hz * t4 + x * (t5_part - t3_part)
        g2 = hx * t1 + hz * t2 - y * (t5_part + t3_part)
        g3 = hy * t2 + hx * t4 + z * t3
        v1, v2, v3 = (feature(k) for k in range(1, 4))
        s = feature(0)
        put(
            0,
            weight(0) * s
            + weight(1) * (x * g1 + y * g2 + z * g3)
            + weight(2) * (x * v1 + y * v2 + z * v3),
        )
        a = weight(3) * s
        w4, w5, w6 = weight(4), weight(5), weight(6)
        p1, p2, p3 = w5 * v1, w5 * v2, w5 * v3
        put(1, a * x + w4 * v1 + (p2 * z - p3 * y) + w6 * g1)
        put(2, a * y + w4 * v2 + (p3 * x - p1 * z) + w6 * g2)
        put(3, a * z + w4 * v3 + (p1 * y - p2 * x) + w6 * g3)
        a = weight(7) * s
        w8, w9 = weight(8), weight(9)
        p1, p2, p3 = w9 * v1 + a * x, w9 * v2 + a * y, w9 * v3 + a * z
        put(4, w8 * t1 + (hy * p1 + hx * p2))
        put(5, w8 * t2 + (hz * p2 + hy * p3))
        put(6, w8 * t3 + (z * p3 - 0.5 * (x * p1 + y * p2)))
        put(7, w8 * t4 + (hz * p1 + hx * p3))
        put(8, w8 * t5 + (hx * p1 - hy * p2))

    def stage(index, held):
        pieces = expansion(index + 1, 1 - held) + reduction(index - 1, 1 - held)
        units = [(lane, group) for lane in range(0, block, 256) for group in range(0, channels, 8)]
        done = 0
        for position, unit in enumerate(units):
            while done < len(pieces) and done * len(units) * 4 < (position + 1) * len(pieces) * 5:
                pieces[done]()
                done += 1
            messages(held, *unit)

    def drain(held):
        for piece in reduction(blocks - 1, held):
            piece()

    for piece in expansion(0, 0):
        piece()

    def visit(index, carry):
        pl.when(2 * index < blocks)(lambda: stage(2 * index, 0))
        pl.when(2 * index + 1 < blocks)(lambda: stage(2 * index + 1, 1))
        return carry

    lax.fori_loop(0, (blocks + 1) // 2, visit, 0)
    odd = lax.rem(blocks, 2)
    pl.when(odd == 1)(lambda: drain(0))
    pl.when(odd == 0)(lambda: drain(1))
    total = sum_sc[0:rows, :] + sum_sc[rows : 2 * rows, :]
    if last:
        total = (total + before_ref[...]) * neighbour_norm
    out_ref[...] = total.astype(out_ref.dtype)


def sum_edges(edge_count, table, edges, hidden, unit, mix, layer_index, column, before=None):
    rows, atoms = table.shape
    slots = edges.shape[1]
    last = before is not None
    block = min(512 if last else 1024, slots)
    paths = mix.shape[1] * mix.shape[2]
    in_vmem = pl.BlockSpec(memory_space=pltpu.VMEM)
    arrays = [edge_count, table, edges, hidden, unit, mix]
    if last:
        arrays.append(before)

    def two(shape, dtype):
        return [pltpu.VMEM(shape, dtype)] * 2

    return pl.pallas_call(
        functools.partial(
            edge_kernel,
            column=column,
            block=block,
            channels=rows // 9,
            layer=layer_index,
            last=last,
        ),
        out_shape=jax.ShapeDtypeStruct((rows, atoms), jnp.bfloat16 if last else jnp.float32),
        in_specs=[pl.BlockSpec(memory_space=pltpu.SMEM)] + [in_vmem] * (len(arrays) - 1),
        out_specs=in_vmem,
        scratch_shapes=two((paths, block), jnp.float32)
        + two((rows, block), jnp.float32)
        + two((2 * rows, block), jnp.bfloat16)
        + two((8, block), jnp.float32)
        + [pltpu.VMEM((atoms, block), jnp.bfloat16), pltpu.VMEM((2 * rows, atoms), jnp.float32)],
        compiler_params=pltpu.CompilerParams(vmem_limit_bytes=40 * 2**20),
        cost_estimate=pl.CostEstimate(
            flops=slots * 400000, bytes_accessed=slots * 300, transcendentals=0
        ),
    )(*arrays)


def total_kernel(
    part_ref, mean_ref, near_sc, far_sc, near_send, near_recv, far_send, far_recv, *, scale
):
    far, *near = SLAB
    sizes = [lax.axis_size(name) for name in near]
    place = [lax.axis_index(name) for name in near]
    far_size = lax.axis_size(far)
    far_place = lax.axis_index(far)
    near_total = math.prod(sizes)

    def split(step):
        return step // (sizes[1] * sizes[2]), step // sizes[2] % sizes[1], step % sizes[2]

    def near_device(step):
        return {
            name: (at + by) % size for name, at, by, size in zip(near, place, split(step), sizes)
        }

    def near_sender(step):
        at = [(p + size - by) % size for p, by, size in zip(place, split(step), sizes)]
        return (at[0] * sizes[1] + at[1]) * sizes[2] + at[2]

    def near_copy(step, slot):
        return pltpu.make_async_remote_copy(
            src_ref=part_ref,
            dst_ref=near_sc.at[slot],
            send_sem=near_send.at[step],
            recv_sem=near_recv.at[slot],
            device_id=near_device(step),
            device_id_type=pl.DeviceIdType.MESH,
        )

    def far_copy(step, slot):
        return pltpu.make_async_remote_copy(
            src_ref=near_sc,
            dst_ref=far_sc.at[slot],
            send_sem=far_send.at[step],
            recv_sem=far_recv.at[slot],
            device_id={far: (far_place + step) % far_size},
            device_id_type=pl.DeviceIdType.MESH,
        )

    barrier = pltpu.get_barrier_semaphore()
    for step in range(1, near_total):
        pl.semaphore_signal(
            barrier, inc=1, device_id=near_device(step), device_id_type=pl.DeviceIdType.MESH
        )
    for step in range(1, far_size):
        pl.semaphore_signal(
            barrier,
            inc=1,
            device_id={far: (far_place + step) % far_size},
            device_id_type=pl.DeviceIdType.MESH,
        )
    pl.semaphore_wait(barrier, near_total + far_size - 2)
    mine = near_sender(0)
    near_sc[mine] = part_ref[...]
    for step in range(1, near_total):
        near_copy(step, mine).start()
    for step in range(1, near_total):
        near_copy(step, near_sender(step)).wait_recv()
    for step in range(1, far_size):
        far_copy(step, far_place).start()
    far_sc[far_place] = near_sc[...]
    for step in range(1, far_size):
        far_copy(step, (far_place + far_size - step) % far_size).wait_recv()
    mean_ref[0, 0] = jnp.sum(far_sc[...]) * scale
    for step in range(1, near_total):
        near_copy(step, mine).wait_send()
    for step in range(1, far_size):
        far_copy(step, far_place).wait_send()


def mean_over_slabs(part, scale):
    lanes = part.shape[1]
    far_size, near_total = lax.axis_size(SLAB[0]), lax.axis_size(SLAB[1:])
    return pl.pallas_call(
        functools.partial(total_kernel, scale=scale),
        out_shape=jax.ShapeDtypeStruct((1, 1), jnp.float32),
        in_specs=[pl.BlockSpec(memory_space=pltpu.VMEM)],
        out_specs=pl.BlockSpec(memory_space=pltpu.SMEM),
        scratch_shapes=[
            pltpu.VMEM((near_total, 1, lanes), jnp.float32),
            pltpu.VMEM((far_size, near_total, 1, lanes), jnp.float32),
            pltpu.SemaphoreType.DMA((near_total,)),
            pltpu.SemaphoreType.DMA((near_total,)),
            pltpu.SemaphoreType.DMA((far_size,)),
            pltpu.SemaphoreType.DMA((far_size,)),
        ],
        compiler_params=pltpu.CompilerParams(collective_id=0, has_side_effects=True),
    )(part)


def local(
    species,
    atom_count,
    halo_index,
    edge_count,
    inner_edges,
    outer_edges,
    inner_vec,
    outer_vec,
    embed_table,
    radial_in,
    radial_mid,
    radial_out,
    mix_in,
    mix_scalar,
    mix_irrep,
    readout,
    species_energy,
):
    atom_total = species.shape[0]
    wide, channels = embed_table.shape[0], mix_in.shape[2]
    rows = 9 * channels
    state_shape = ((9, wide, atom_total), jnp.float32)
    table_shapes = [((rows, atom_total), jnp.bfloat16)]
    table_shapes += [((rows, halo_index.shape[2]), jnp.bfloat16)] * 2
    gathered = (9, wide, atom_total)
    species = species[None]
    layers = radial_in.shape[0]
    node_state, table, to_left, to_right = node_call(
        start_kernel,
        [],
        [species, embed_table, mix_in, halo_index],
        [state_shape, *table_shapes],
    )
    nets = radial_net(edge_count, inner_vec, outer_vec, radial_in, radial_mid)
    for layer in range(layers):
        from_left = passed_along(to_right, SLAB, 1)
        from_right = passed_along(to_left, SLAB, -1)
        summed = sum_edges(edge_count, table, inner_edges, *nets[0:2], radial_out, layer, 0)
        halo_table = jnp.concatenate([from_left, from_right], axis=1)
        own = sum_edges(
            edge_count, halo_table, outer_edges, *nets[2:4], radial_out, layer, 1, summed
        )
        other = lax.ppermute(own, "chan", [(0, 1), (1, 0)])
        arrays = [own, other, node_state, mix_scalar, mix_irrep]
        if layer + 1 < layers:
            node_state, table, to_left, to_right = node_call(
                functools.partial(middle_kernel, layer=layer),
                [],
                [*arrays, mix_in, halo_index],
                [state_shape, *table_shapes],
                gathered,
            )
        else:
            node_state, atom_energy, part = node_call(
                functools.partial(final_kernel, layer=layer),
                [atom_count, species_energy],
                [*arrays, readout[:, None], species],
                [state_shape, ((1, atom_total), jnp.float32), ((1, 128), jnp.float32)],
                gathered,
            )
    mean = mean_over_slabs(part, 1.0 / (atom_total * lax.axis_size(SLAB)))
    return (node_state, atom_energy[0], mean[0, 0])


def solution(mesh):
    finer = Mesh(
        mesh.devices.reshape(8, 2, 4, 2, mesh.shape["chan"]),
        ("slab_0", "slab_1", "slab_2", "slab_3", "chan"),
    )
    placed = (
        P(SLAB),
        P(SLAB),
        P(SLAB, None, None),
        P(SLAB, None),
        P(None, SLAB),
        P(None, SLAB),
        P(None, SLAB),
        P(None, SLAB),
        P(),
        P(),
        P(),
        P(None, None, "chan", None),
        P(None, None, "chan", None),
        P(),
        P(),
        P(),
        P(),
    )
    return jax.shard_map(
        local,
        mesh=finer,
        in_specs=placed,
        out_specs=(P(None, None, SLAB), P(SLAB), P()),
        check_vma=False,
    )
```
